32 devices in a mesh: gx: 4 (over x, core), gy: 4 (over z), gz: 2 (over y).
Axes of the slice: x: 2, y: 2, z: 4, core: 2. Of those that a mesh axis runs over, the one named last changes fastest.
Arguments:
- attn_out: bfloat16 [704, 8192], P('gx', ('gz', 'gy')), may hold values from -6 to 6
- residual: bfloat16 [704, 8192], P('gx', ('gy', 'gz')), may hold values from -60 to 60
- proj_weight: bfloat16 [8192, 8192], P(('gz', 'gx'), 'gy'), may hold values from -0.0625 to 0.0625
- norm_gain: float32 [8192], P(('gy', 'gz')), may hold values from 0.1 to 1.9
- gate_proj: bfloat16 [8192, 14336], P(('gy', 'gx'), 'gz'), may hold values from -0.0625 to 0.0625
- up_proj: bfloat16 [8192, 14336], P(('gy', 'gx'), 'gz'), may hold values from -0.0625 to 0.0625
- down_proj: bfloat16 [14336, 8192], P(('gz', 'gx'), 'gy'), may hold values from -0.046875 to 0.046875
Outputs:
- layer_out: bfloat16 [704, 8192], P('gx', ('gy', 'gz'))
The draws below stay inside these ranges and needn't reach their ends.
All inputs are finite; a program needn't handle non-finite values.
Results may differ from the reference program's by a relative error of at most 0.0029.
Values may be sent and summed in bfloat16 or wider, within the bound.
A program may use at most 128 MiB of HBM per device.

```python
import jax
import jax.numpy as jnp
from jax import lax

D = 8192
FFW = 14336
TOKENS = 704


def draw_residual(key, part):
    first, second = jax.random.split(key, 2)
    ramp = 1.0 + 2.0 * jnp.arange(D, dtype=jnp.float32)[None, :] / (D - 1)
    values = jnp.clip(jax.random.normal(first, (TOKENS, D), jnp.float32), -6.0, 6.0)
    scales = jnp.exp(jax.random.uniform(second, (TOKENS, 1), jnp.float32, jnp.log(0.3), jnp.log(3.0)))
    return (values * scales * ramp).astype(jnp.bfloat16)


def block_scale(rng, shape, shards, smallest, high):
    loudness, own = 1.0, jax.random.fold_in(rng, 6)
    for dim, parts in shards:
        steps = jnp.exp(jax.random.uniform(jax.random.fold_in(own, dim), (parts,), jnp.float32, smallest / len(shards), high / len(shards)))
        loudness = loudness * jnp.repeat(steps, shape[dim] // parts).reshape([-1 if axis == dim else 1 for axis in range(len(shape))])
    return loudness


def centred(rng, extent, scale, reach, cuts=(), held_as=jnp.bfloat16):
    factor_of = block_scale(rng, extent, cuts, -0.22, 0.18) if cuts else 1.0
    result = jax.random.normal(rng, extent, jnp.float32) * scale * factor_of
    return jnp.minimum(jnp.maximum(result, -reach), reach).astype(held_as)


def setup_inputs(seed: int = 0) -> dict:
    key_of = jax.random.split(jax.random.key(seed), 8)
    return {
        "attn_out": centred(key_of[0], (TOKENS, D), 1.0, 6.0, ((0, 4), (1, 8))),
        "residual": draw_residual(jax.random.fold_in(key_of[7], 71), 0),
        "proj_weight": centred(key_of[2], (D, D), D ** -0.5, 0.0625, ((0, 8), (1, 4))),
        "norm_gain": jnp.clip(1.0 + 0.18 * jax.random.normal(key_of[3], (D,), jnp.float32), 0.1, 1.9),
        "gate_proj": centred(key_of[4], (D, FFW), D ** -0.5, 0.0625, ((0, 16), (1, 2))),
        "up_proj": centred(key_of[5], (D, FFW), D ** -0.5, 0.0625, ((0, 16), (1, 2))),
        "down_proj": centred(key_of[6], (FFW, D), FFW ** -0.5, 0.046875, ((0, 8), (1, 4))),
    }


def reference(attn_out, residual, proj_weight, norm_gain, gate_proj, up_proj, down_proj):
    projected = jnp.dot(attn_out, proj_weight, preferred_element_type=jnp.float32)
    stream = residual.astype(jnp.float32) + projected
    inverse = lax.rsqrt(lax.optimization_barrier(jnp.mean(stream * stream, axis=1, keepdims=True)) + 1e-05)
    scaled = (stream * norm_gain.astype(jnp.float32)[None, :]).astype(jnp.bfloat16)
    gate_sum = inverse * jnp.dot(scaled, gate_proj, preferred_element_type=jnp.float32)
    up_sum = inverse * jnp.dot(scaled, up_proj, preferred_element_type=jnp.float32)
    hidden = (jax.nn.silu(gate_sum) * up_sum).astype(jnp.bfloat16)
    down_sum = jnp.dot(hidden, down_proj, preferred_element_type=jnp.float32)
    return (stream + down_sum).astype(jnp.bfloat16)
```

```python
import jax
import jax.numpy as jnp
from jax import lax
from jax.sharding import PartitionSpec as P


def product(left, right):
    return jnp.dot(left, right, preferred_element_type=jnp.float32)


def swapped(value, axis, size, bit):
    return lax.ppermute(value, axis, [(i, i ^ bit) for i in range(size)])


def halved(blocks, axis, size, bit, rel=0):
    if bit == 1:
        return blocks(rel)
    bit //= 2
    away = halved(blocks, axis, size, bit, rel | bit).astype(jnp.bfloat16)
    return halved(blocks, axis, size, bit, rel) + swapped(away, axis, size, bit).astype(jnp.float32)


def reduced(blocks, axis, size):
    return halved(blocks, axis, size, size)


def on_device(sizes, attn_out, residual, proj_weight, norm_gain, gate_proj, up_proj, down_proj):
    gx, gy, gz = sizes
    assert gx == gy
    rows, home = residual.shape
    width = home * gy * gz
    x, z = lax.axis_index("gx"), lax.axis_index("gz")

    turn = [(i * gy + j, j * gy + i) for i in range(gx) for j in range(gy)]
    turned = lax.ppermute(attn_out, ("gx", "gy"), turn)
    cut = turned.shape[1] // 2
    attn_cols = [
        lax.all_gather(turned[:, at:at + cut], "gy", axis=0, tiled=True) for at in (0, cut)
    ]

    def scattered(lefts, weight):
        done, total = 0, None
        for left in lefts:
            depth = left.shape[1]
            part = product(left, lax.slice_in_dim(weight, done, done + depth, axis=0))
            done += depth
            total = part if total is None else total + part

        def columns(zrel):
            def term(xrel):
                at = ((x ^ xrel) * rows, (z ^ zrel) * home)
                return lax.dynamic_slice(total, at, (rows, home))
            return reduced(term, "gx", gx)
        return reduced(columns, "gz", gz)

    projected = scattered(attn_cols, proj_weight)
    stream = residual.astype(jnp.float32) + projected
    scaled = (stream * norm_gain[None, :]).astype(jnp.bfloat16)
    scaled = lax.all_gather(scaled, "gz", axis=1, tiled=True)
    scaled = lax.all_to_all(scaled, "gx", split_axis=1, concat_axis=0, tiled=True)

    squares = jnp.sum(stream * stream, axis=1)
    for axis, size in (("gy", gy), ("gz", gz)):
        bit = 1
        while bit < size:
            squares = squares + swapped(squares, axis, size, bit)
            bit *= 2
    squares = lax.ppermute(squares, ("gx", "gy"), turn)
    inverse = lax.rsqrt(squares / width + 1e-05)[:, None]

    block = gate_proj.shape[1] // gx
    head = 3 * block // 7
    top = gx // 2

    def term_of(weight, at, size, left):
        def term(rel):
            return product(
                left, lax.dynamic_slice_in_dim(weight, (x ^ rel) * block + at, size, 1)
            )
        return term

    def far(at, size, left):
        return [
            halved(term_of(weight, at, size, left), "gx", gx, top, top).astype(jnp.bfloat16)
            for weight in (gate_proj, up_proj)
        ]

    def joined(at, size, left, arrived):
        parts = [
            (halved(term_of(weight, at, size, left), "gx", gx, top) + part.astype(jnp.float32))
            for weight, part in zip((gate_proj, up_proj), arrived)
        ]
        return jnp.concatenate([part.astype(jnp.bfloat16) for part in parts], axis=1)

    def activated(both):
        both = lax.psum_scatter(both, "gy", scatter_dimension=0, tiled=True).astype(jnp.float32)
        half = both.shape[1] // 2
        gate_sum, up_sum = inverse * both[:, :half], inverse * both[:, half:]
        piece = (jax.nn.silu(gate_sum) * up_sum).astype(jnp.bfloat16)
        return lax.all_gather(piece, "gy", axis=0, tiled=True)

    first = [swapped(part, "gx", gx, top) for part in far(0, head, scaled)]
    second = far(head, block - head, scaled)
    first, second = lax.optimization_barrier((first, second))
    second = [swapped(part, "gx", gx, top) for part in second]
    early = activated(joined(0, head, scaled, first))
    late = joined(head, block - head, scaled, second)
    early, late = lax.optimization_barrier((early, late))
    hidden = [early, activated(late)]

    down_sum = scattered(hidden, down_proj)
    return (stream + down_sum).astype(jnp.bfloat16)


def solution(mesh):
    sizes = tuple(mesh.shape[name] for name in ("gx", "gy", "gz"))
    in_specs = (
        P("gx", ("gz", "gy")),
        P("gx", ("gy", "gz")),
        P(("gz", "gx"), "gy"),
        P(("gy", "gz")),
        P(("gy", "gx"), "gz"),
        P(("gy", "gx"), "gz"),
        P(("gz", "gx"), "gy"),
    )
    out_specs = P("gx", ("gy", "gz"))
    return jax.shard_map(
        lambda *args: on_device(sizes, *args),
        mesh=mesh, in_specs=in_specs, out_specs=out_specs, check_vma=False,
    )
```
